32 devices in a mesh: gx: 8 (over z, x), gy: 4 (over y, core).
Axes of the slice: x: 2, y: 2, z: 4, core: 2. Of those that a mesh axis runs over, the one named last changes fastest.
Arguments:
- gradient: float32 [1024, 128], P('gx', 'gy'), may hold values from -6 to 6
- stat_old: float32 [1024, 1024], P('gx', 'gy'), may hold values from -1.001 to 1.001, as said below
Outputs:
- statistic: float32 [1024, 1024], P('gx', 'gy')
- inverse_root: float32 [1024, 1024], P('gx', 'gy')
The draws below stay inside these ranges and needn't reach their ends.
Inputs may be any that keep to these rules, and one draw needn't show every extreme that they name: stat_old is symmetric positive semidefinite with unit diagonal, the Gram matrix of 1024 unit-length rows of 256 entries.
All inputs are finite; a program needn't handle non-finite values.
Results may differ from the reference program's by a relative error of at most 0.0003.
Values sent between devices are 32-bit elements.
A program may use at most 64 MiB of HBM per device.

```python
import jax
import jax.numpy as jnp
from jax import lax

NSIDE = 1024
MCOLS = 128


def draw_stat_old(key, part):
    factor = jax.random.normal(key, (NSIDE, NSIDE // 4), jnp.float32)
    lengths = jnp.sqrt(jnp.sum(factor * factor, axis=1, keepdims=True))
    factor = factor / lengths
    return jnp.dot(factor, factor.T, preferred_element_type=jnp.float32, precision=lax.Precision.HIGHEST)


def steps_of(stream_key, dims, pieces, low, high):
    factor_of = 1.0
    for dim, shards_of in pieces:
        draws = jax.random.uniform(jax.random.fold_in(jax.random.fold_in(stream_key, 6), dim), (shards_of,), jnp.float32, low / len(pieces), high / len(pieces))
        factor_of = factor_of * jnp.repeat(jnp.exp(draws), dims[dim] // shards_of).reshape((-1,) + (1,) * (len(dims) - 1 - dim))
    return factor_of


def bell_draw(rng, dims, width, reach, pieces=(), kind=jnp.bfloat16):
    array = jax.random.normal(rng, dims, jnp.float32) * width
    if len(pieces) > 0:
        array = steps_of(rng, dims, pieces, -0.22, 0.18) * array
    return jnp.clip(array, min=-reach, max=reach).astype(kind)


def setup_inputs(seed: int = 0) -> dict:
    key_of = jax.random.split(jax.random.key(seed), 3)
    return {
        "gradient": bell_draw(key_of[0], (NSIDE, MCOLS), 1.0, 6.0, ((0, 8), (1, 4)), jnp.float32),
        "stat_old": draw_stat_old(jax.random.fold_in(key_of[2], 71), 0),
    }


def matmul(leading, trailing):
    return jnp.dot(leading, trailing, preferred_element_type=jnp.float32, precision=lax.Precision.HIGHEST)

def reference(gradient, stat_old):
    statistic = 0.9 * stat_old + matmul(gradient, gradient.T) / MCOLS
    divisor = 2.0 * jnp.sqrt(jnp.sum(statistic * statistic) / NSIDE)
    identity = jnp.eye(NSIDE, dtype=jnp.float32)
    normed = statistic / divisor
    first_step = 1.5 * identity - 0.5 * normed
    root_half = matmul(normed, first_step)
    product_mid = matmul(first_step, root_half)
    second_step = 1.5 * identity - 0.5 * product_mid
    inverse_root = matmul(second_step, first_step)
    return (statistic, inverse_root)
```

```python
import jax
import jax.numpy as jnp
from jax import lax
from jax.sharding import PartitionSpec as P


def matmul(leading, trailing, precision):
    return jnp.dot(leading, trailing, preferred_element_type=jnp.float32, precision=precision)


def whole(block):
    rows = lax.all_gather(block, "gy", axis=1, tiled=True)
    return lax.all_gather(rows, "gx", axis=0, tiled=True)


def local(gradient, stat_old):
    height, width = stat_old.shape
    row_start = lax.axis_index("gx") * height
    col_start = lax.axis_index("gy") * width
    grad = whole(gradient)
    stat = whole(stat_old)
    high = lax.Precision.HIGH
    full = 0.9 * stat + matmul(grad, grad.T, high) / grad.shape[1]
    side = full.shape[0]
    row_panel = lax.dynamic_slice_in_dim(full, row_start, height, 0)
    col_panel = lax.dynamic_slice_in_dim(full, col_start, width, 1)
    statistic = lax.dynamic_slice_in_dim(row_panel, col_start, width, 1)
    scale = 0.5 * lax.rsqrt(jnp.sum(full * full) / side)
    square_rows = matmul(row_panel, full, high)
    square_cols = matmul(full, col_panel, high)

    def eye(shape, first_row, first_col):
        rows = first_row + lax.broadcasted_iota(jnp.int32, shape, 0)
        cols = first_col + lax.broadcasted_iota(jnp.int32, shape, 1)
        return (rows == cols).astype(jnp.float32)

    def quad(square, panel, first_row, first_col):
        ident = eye(square.shape, first_row, first_col)
        return (0.25 * scale * scale) * square - (1.125 * scale) * panel + 0.84375 * ident

    left = quad(square_rows, row_panel, row_start, 0)
    right = quad(square_cols, col_panel, 0, col_start)
    ident = eye(statistic.shape, row_start, col_start)
    inverse_root = matmul(left, right, high) - (0.5390625 * scale) * statistic + 1.5380859375 * ident
    return (statistic, inverse_root)


def solution(mesh):
    return jax.shard_map(
        local,
        mesh=mesh,
        in_specs=(P("gx", "gy"), P("gx", "gy")),
        out_specs=(P("gx", "gy"), P("gx", "gy")),
        check_vma=False,
    )
```

```python
import functools

import jax
import jax.numpy as jnp
from jax import lax
from jax.experimental import pallas as pl
from jax.experimental.pallas import tpu as pltpu
from jax.sharding import PartitionSpec as P

MESH = pl.DeviceIdType.MESH


def split(value):
    high = value.astype(jnp.bfloat16)
    return high, (value - high.astype(jnp.float32)).astype(jnp.bfloat16)


def dot3(left, right, dims):
    def one(a, b):
        return lax.dot_general(a, b, (dims, ((), ())), preferred_element_type=jnp.float32)

    return one(left[0], right[0]) + (one(left[0], right[1]) + one(left[1], right[0]))


def kernel(
    R, C, pay_ref, stat_ref, stat_out, root_out,
    buf, gt_hi, gt_lo, g_hi, g_lo, s_hi, s_lo, l_hi, l_lo, q_hi, q_lo, acc,
    send_sem, recv_sem, pair_sem, own_sem,
):
    height, width = stat_ref.shape
    payload = pay_ref.shape[0]
    part = payload // 2
    side = R * height
    X, Z, Y = 2, R // 2, C // 2
    row, col = lax.axis_index("gx"), lax.axis_index("gy")
    z, x, y, core = row // X, row % X, col // 2, col % 2
    x_other = 1 - x
    z_at = [z] + [lax.rem(z + k, Z) for k in range(1, Z)]
    y_at = [y] + [lax.rem(y + k, Y) for k in range(1, Y)]
    z_order = [k for pair in zip(range(1, Z), range(Z - 1, 0, -1)) for k in pair]
    z_order = list(dict.fromkeys(z_order))

    barrier = pltpu.get_barrier_semaphore()
    peers = [(z_at[k] * X + x, col) for k in range(1, Z)]
    peers += [(z * X + x_other, col)]
    peers += [(row, y_at[k] * 2 + core) for k in range(1, Y)]
    peers += [(row, y * 2 + (1 - core))]
    for peer in peers:
        pl.semaphore_signal(barrier, inc=1, device_id=peer, device_id_type=MESH)
    pl.semaphore_wait(barrier, len(peers))

    started = []

    def place(zz, xx, yy, cc, h):
        return buf.at[yy * 2 + cc, zz * X + xx, pl.ds(h * part, part), :]

    def slot(zz, xx, yy, h):
        return ((h * Z + zz) * X + xx) * Y + yy

    def send(src, zz, xx, yy, h, peer, arrive):
        copy = pltpu.make_async_remote_copy(
            src_ref=src,
            dst_ref=place(zz, xx, yy, core, h),
            send_sem=send_sem.at[len(started)],
            recv_sem=arrive.at[slot(zz, xx, yy, h)],
            device_id=peer,
            device_id_type=MESH,
        )
        copy.start()
        started.append(copy)

    def source(zz, xx, yy, h, own):
        return pay_ref.at[pl.ds(h * part, part), :] if own else place(zz, xx, yy, core, h)

    def to_x(zz, yy, h, own=False):
        send(source(zz, x, yy, h, own), zz, x, yy, h, (z * X + x_other, col), recv_sem)

    def to_y(zz, xx, h, own=False):
        for k in range(1, Y):
            send(source(zz, xx, y, h, own), zz, xx, y, h, (row, y_at[k] * 2 + core), recv_sem)

    def to_pair(zz, xx, yy, h, own=False):
        send(source(zz, xx, yy, h, own), zz, xx, yy, h, (row, y * 2 + (1 - core)), pair_sem)

    def arrived(zz, xx, yy, cc, h, sem):
        here = place(zz, xx, yy, cc, h)
        pltpu.make_async_copy(here, here, sem.at[slot(zz, xx, yy, h)]).wait()

    own_copy = pltpu.make_async_copy(pay_ref, buf.at[col, row], own_sem)
    own_copy.start()
    to_x(z, y, 0, True)
    to_y(z, x, 1, True)
    for k in z_order:
        for h in range(2):
            send(source(z, x, y, h, True), z, x, y, h, (z_at[k] * X + x, col), recv_sem)
    to_x(z, y, 1, True)
    to_y(z, x, 0, True)
    for h in range(2):
        to_pair(z, x, y, h, True)

    def second_leg(zz):
        arrived(zz, x_other, y, core, 0, recv_sem)
        to_y(zz, x_other, 0)
        to_pair(zz, x_other, y, 0)
        for k in range(1, Y):
            arrived(zz, x, y_at[k], core, 1, recv_sem)
            to_x(zz, y_at[k], 1)
            to_pair(zz, x, y_at[k], 1)

    second_leg(z)
    for k in z_order:
        zz = z_at[k]
        for h in range(2):
            arrived(zz, x, y, core, h, recv_sem)
        to_x(zz, y, 0)
        to_y(zz, x, 1)
        to_x(zz, y, 1)
        to_y(zz, x, 0)
        for h in range(2):
            to_pair(zz, x, y, h)
    for k in z_order:
        second_leg(z_at[k])
    for k in [0] + z_order:
        zz = z_at[k]
        arrived(zz, x_other, y, core, 1, recv_sem)
        to_pair(zz, x_other, y, 1)
        for k in range(1, Y):
            arrived(zz, x, y_at[k], core, 0, recv_sem)
            to_pair(zz, x, y_at[k], 0)
    for k in [0] + z_order:
        zz = z_at[k]
        for k in range(1, Y):
            for h in range(2):
                arrived(zz, x_other, y_at[k], core, h, recv_sem)
                to_pair(zz, x_other, y_at[k], h)
    for k in [0] + z_order:
        for xx in range(X):
            for yy in range(Y):
                for h in range(2):
                    arrived(z_at[k], xx, yy, 1 - core, h, pair_sem)
    own_copy.wait()

    pieces = width // height
    step = payload - height
    for i in range(R):
        for j in range(C):
            for l in range(pieces):
                at = (j * pieces + l) * step
                value = buf[j, i, height:, l * height:(l + 1) * height]
                high, low = split(value)
                gt_hi[at:at + step, i * height:(i + 1) * height] = high
                gt_lo[at:at + step, i * height:(i + 1) * height] = low
    depth = gt_hi.shape[0]

    def turn(i, carry):
        here = pl.ds(pl.multiple_of(i * height, height), height)
        g_hi[here, :] = gt_hi[:, here].T
        g_lo[here, :] = gt_lo[:, here].T
        return carry

    lax.fori_loop(0, R, turn, 0)

    def outer(here, there):
        return dot3(
            (g_hi[here, :], g_lo[here, :]), (gt_hi[:, there], gt_lo[:, there]), ((1,), (0,))
        ) * (1.0 / depth)

    acc[...] = jnp.zeros_like(acc)

    def assemble(i, carry):
        here = pl.ds(pl.multiple_of(i * height, height), height)
        for j in range(C):
            there = slice(j * width, (j + 1) * width)
            value = 0.9 * buf[j, i, :height, :] + outer(here, there)
            acc[...] += value * value
            high, low = split(value)
            s_hi[here, there] = high
            s_lo[here, there] = low
        return carry

    lax.fori_loop(0, R, assemble, 0)
    my_rows = pl.ds(pl.multiple_of(row * height, height), height)
    my_cols = pl.ds(pl.multiple_of(col * width, width), width)
    statistic = 0.9 * stat_ref[...] + outer(my_rows, my_cols)
    stat_out[...] = statistic
    total = jnp.sum(jnp.sum(acc[...], axis=0, keepdims=True), axis=1, keepdims=True)
    scale = 0.5 / jnp.sqrt(total / side)

    for store, kept in ((l_hi, s_hi), (l_lo, s_lo)):
        store[:height, :] = kept[my_rows, :]
        store[height:, :] = kept[my_cols, :]

    left_rows = height + width
    line = lax.broadcasted_iota(jnp.int32, (left_rows, width), 0)
    line = jnp.where(line < height, row * height + line, col * width + line - height)
    across = lax.broadcasted_iota(jnp.int32, (left_rows, width), 1)

    def square(j, carry):
        there = pl.ds(pl.multiple_of(j * width, width), width)
        value = dot3((l_hi[...], l_lo[...]), (s_hi[:, there], s_lo[:, there]), ((1,), (0,)))
        panel = l_hi[:, there].astype(jnp.float32) + l_lo[:, there].astype(jnp.float32)
        ident = jnp.where(line == across + j * width, 0.84375, 0.0)
        quad = (0.25 * scale * scale) * value - (1.125 * scale) * panel + ident
        high, low = split(quad)
        q_hi[:, there] = high
        q_lo[:, there] = low
        return carry

    lax.fori_loop(0, C, square, 0)
    root = dot3(
        (q_hi[:height, :], q_lo[:height, :]), (q_hi[height:, :], q_lo[height:, :]), ((1,), (1,))
    )
    rows = row * height + lax.broadcasted_iota(jnp.int32, (height, width), 0)
    cols = col * width + lax.broadcasted_iota(jnp.int32, (height, width), 1)
    root_out[...] = (
        root - (0.5390625 * scale) * statistic + jnp.where(rows == cols, 1.5380859375, 0.0)
    )
    for copy in started:
        copy.wait_send()


def local(R, C, gradient, stat_old):
    height, width = stat_old.shape
    pieces = width // height
    lines = gradient.shape[1] // pieces
    turned = gradient.T
    extra = jnp.concatenate([turned[l * lines:(l + 1) * lines] for l in range(pieces)], axis=1)
    pay = jnp.concatenate([stat_old, extra], axis=0)
    payload = pay.shape[0]
    side, depth = R * height, C * gradient.shape[1]
    Z, X, Y = R // 2, 2, C // 2
    chips = Z * X * Y
    sends = 2 * (Z - 1) + 2 * Z + Z * (Y - 1) + (3 * Z) * (Y - 1) + 2 * chips
    half = jnp.bfloat16
    vmem = pl.BlockSpec(memory_space=pltpu.VMEM)
    return pl.pallas_call(
        functools.partial(kernel, R, C),
        out_shape=(jax.ShapeDtypeStruct(stat_old.shape, jnp.float32),) * 2,
        in_specs=[vmem] * 2,
        out_specs=(vmem,) * 2,
        scratch_shapes=[
            pltpu.VMEM((C, R, payload, width), jnp.float32),
            pltpu.VMEM((depth, side), half),
            pltpu.VMEM((depth, side), half),
            pltpu.VMEM((side, depth), half),
            pltpu.VMEM((side, depth), half),
            pltpu.VMEM((side, side), half),
            pltpu.VMEM((side, side), half),
            pltpu.VMEM((height + width, side), half),
            pltpu.VMEM((height + width, side), half),
            pltpu.VMEM((height + width, side), half),
            pltpu.VMEM((height + width, side), half),
            pltpu.VMEM((height, width), jnp.float32),
            pltpu.SemaphoreType.DMA((sends,)),
            pltpu.SemaphoreType.DMA((2 * chips,)),
            pltpu.SemaphoreType.DMA((2 * chips,)),
            pltpu.SemaphoreType.DMA,
        ],
        compiler_params=pltpu.CompilerParams(collective_id=0, has_side_effects=True),
    )(pay, stat_old)


def solution(mesh):
    return jax.shard_map(
        functools.partial(local, mesh.shape["gx"], mesh.shape["gy"]),
        mesh=mesh,
        in_specs=(P("gx", "gy"), P("gx", "gy")),
        out_specs=(P("gx", "gy"), P("gx", "gy")),
        check_vma=False,
    )
```

```python
import functools

import jax
import jax.numpy as jnp
from jax import lax
from jax.experimental import pallas as pl
from jax.experimental.pallas import tpu as pltpu
from jax.sharding import PartitionSpec as P

MESH = pl.DeviceIdType.MESH


def split(value):
    high = value.astype(jnp.bfloat16)
    return high, (value - high.astype(jnp.float32)).astype(jnp.bfloat16)


def dot3(left, right, dims):
    def one(a, b):
        return lax.dot_general(a, b, (dims, ((), ())), preferred_element_type=jnp.float32)

    return one(left[0], right[0]) + (one(left[0], right[1]) + one(left[1], right[0]))


def mirror(R, C, height, width):
    return width == 2 * height and R == 2 * C


def chosen(i, j):
    odd = i % 2
    return jnp.where(i >= 2 * j, odd, 1 - odd)


def kernel(
    R, C, pay_ref, stat_ref, stat_out, root_out,
    buf, spare, gt, g, s_hi, s_lo, l_hi, l_lo, q_hi, q_lo, acc,
    send_sem, recv_sem, pair_sem, own_sem, spare_send, spare_recv, spare_pair,
):
    height, width = stat_ref.shape
    payload = pay_ref.shape[0]
    part = payload // 2
    side = R * height
    mirrored = mirror(R, C, height, width)
    X, Z, Y = 2, R // 2, C // 2
    row, col = lax.axis_index("gx"), lax.axis_index("gy")
    z, x, y, core = row // X, row % X, col // 2, col % 2
    x_other = 1 - x
    z_at = [z] + [lax.rem(z + k, Z) for k in range(1, Z)]
    y_at = [y] + [lax.rem(y + k, Y) for k in range(1, Y)]
    z_order = [k for pair in zip(range(1, Z), range(Z - 1, 0, -1)) for k in pair]
    z_order = list(dict.fromkeys(z_order))

    barrier = pltpu.get_barrier_semaphore()
    peers = [(z_at[k] * X + x, col) for k in range(1, Z)]
    peers += [(z * X + x_other, col)]
    peers += [(row, y_at[k] * 2 + core) for k in range(1, Y)]
    peers += [(row, y * 2 + (1 - core))]
    for peer in peers:
        pl.semaphore_signal(barrier, inc=1, device_id=peer, device_id_type=MESH)
    pl.semaphore_wait(barrier, len(peers))

    started = []

    def place(zz, xx, yy, cc, h):
        return buf.at[yy * 2 + cc, zz * X + xx, pl.ds(h * part, part), :]

    def slot(zz, xx, yy, h):
        return ((h * Z + zz) * X + xx) * Y + yy

    def both(zz, xx, yy, cc):
        return jnp.logical_and(xx == 0, yy * 2 + cc == zz)

    def spare_place(zz, h):
        return spare.at[zz, pl.ds(h * (height // 2), height // 2), :]

    def send(src, zz, xx, yy, h, peer, pair=False):
        copy = pltpu.make_async_remote_copy(
            src_ref=src,
            dst_ref=place(zz, xx, yy, core, h),
            send_sem=send_sem.at[len(started)],
            recv_sem=(pair_sem if pair else recv_sem).at[slot(zz, xx, yy, h)],
            device_id=peer,
            device_id_type=MESH,
        )
        copy.start()
        more = None
        if mirrored:
            own = src is not None and src_is_own[0]
            start = (
                stat_ref.at[pl.ds(h * (height // 2), height // 2), pl.ds(height, height)]
                if own
                else spare_place(zz, h)
            )
            more = pltpu.make_async_remote_copy(
                src_ref=start,
                dst_ref=spare_place(zz, h),
                send_sem=spare_send.at[len(started)],
                recv_sem=(spare_pair if pair else spare_recv).at[h * Z + zz],
                device_id=peer,
                device_id_type=MESH,
            )
            pl.when(both(zz, xx, yy, core))(more.start)
        started.append((copy, more, both(zz, xx, yy, core)))

    src_is_own = [False]

    def source(zz, xx, yy, h, own):
        src_is_own[0] = own
        return pay_ref.at[pl.ds(h * part, part), :] if own else place(zz, xx, yy, core, h)

    def to_x(zz, yy, h, own=False):
        send(source(zz, x, yy, h, own), zz, x, yy, h, (z * X + x_other, col))

    def to_y(zz, xx, h, own=False):
        for k in range(1, Y):
            send(source(zz, xx, y, h, own), zz, xx, y, h, (row, y_at[k] * 2 + core))

    def to_pair(zz, xx, yy, h, own=False):
        send(source(zz, xx, yy, h, own), zz, xx, yy, h, (row, y * 2 + (1 - core)), True)

    def arrived(zz, xx, yy, cc, h, sem):
        here = place(zz, xx, yy, cc, h)
        pltpu.make_async_copy(here, here, sem.at[slot(zz, xx, yy, h)]).wait()
        if mirrored:
            there = spare_place(zz, h)
            sems = spare_pair if sem is pair_sem else spare_recv
            more = pltpu.make_async_copy(there, there, sems.at[h * Z + zz])
            pl.when(both(zz, xx, yy, cc))(more.wait)

    own_copy = pltpu.make_async_copy(pay_ref, buf.at[col, row], own_sem.at[0])
    own_copy.start()
    if mirrored:
        own_more = pltpu.make_async_copy(
            stat_ref.at[:, pl.ds(height, height)], spare.at[z], own_sem.at[1]
        )
        pl.when(both(z, x, y, core))(own_more.start)
    to_x(z, y, 0, True)
    to_y(z, x, 1, True)
    for k in z_order:
        for h in range(2):
            send(source(z, x, y, h, True), z, x, y, h, (z_at[k] * X + x, col))
    to_x(z, y, 1, True)
    to_y(z, x, 0, True)
    for h in range(2):
        to_pair(z, x, y, h, True)

    def second_leg(zz):
        arrived(zz, x_other, y, core, 0, recv_sem)
        to_y(zz, x_other, 0)
        to_pair(zz, x_other, y, 0)
        for k in range(1, Y):
            arrived(zz, x, y_at[k], core, 1, recv_sem)
            to_x(zz, y_at[k], 1)
            to_pair(zz, x, y_at[k], 1)

    second_leg(z)
    for k in z_order:
        zz = z_at[k]
        for h in range(2):
            arrived(zz, x, y, core, h, recv_sem)
        to_x(zz, y, 0)
        to_y(zz, x, 1)
        to_x(zz, y, 1)
        to_y(zz, x, 0)
        for h in range(2):
            to_pair(zz, x, y, h)
    for k in z_order:
        second_leg(z_at[k])
    for k in [0] + z_order:
        zz = z_at[k]
        arrived(zz, x_other, y, core, 1, recv_sem)
        to_pair(zz, x_other, y, 1)
        for k in range(1, Y):
            arrived(zz, x, y_at[k], core, 0, recv_sem)
            to_pair(zz, x, y_at[k], 0)
    for k in [0] + z_order:
        zz = z_at[k]
        for k in range(1, Y):
            for h in range(2):
                arrived(zz, x_other, y_at[k], core, h, recv_sem)
                to_pair(zz, x_other, y_at[k], h)
    for k in [0] + z_order:
        for xx in range(X):
            for yy in range(Y):
                for h in range(2):
                    arrived(z_at[k], xx, yy, 1 - core, h, pair_sem)
    own_copy.wait()
    if mirrored:
        pl.when(both(z, x, y, core))(own_more.wait)

    step = payload - height
    depth = C * step
    for i in range(R):
        for j in range(C):
            at = j * step
            here = slice(i * height, (i + 1) * height)
            high, low = split(buf[j, i, height:, :])
            gt[at:at + step, here] = high
            gt[depth + at:depth + at + step, here] = low
            gt[2 * depth + at:2 * depth + at + step, here] = high

    def turn(i, carry):
        here = pl.ds(pl.multiple_of(i * height, height), height)
        high = gt[:depth, here].T
        g[here, :depth] = high
        g[here, depth:2 * depth] = high
        g[here, 2 * depth:] = gt[depth:2 * depth, here].T
        return carry

    lax.fori_loop(0, R, turn, 0)

    def outer(here, there):
        return jnp.dot(g[here, :], gt[:, there], preferred_element_type=jnp.float32) * (1.0 / depth)

    acc[...] = jnp.zeros_like(acc)

    def put(value, a, b):
        here = pl.ds(pl.multiple_of(a * height, height), height)
        there = pl.ds(pl.multiple_of(b * height, height), height)
        value = 0.9 * value + outer(here, there)
        times = jnp.where(a == b, 1.0, 2.0) if mirrored else 1.0
        acc[...] += times * (value * value)
        high, low = split(value)
        s_hi[here, there] = high
        s_lo[here, there] = low
        if mirrored:
            s_hi[there, here] = high.T
            s_lo[there, here] = low.T

    def assemble(i, carry):
        for j in range(C):
            put(buf[j, i, :height, :], i, 2 * j + chosen(i, j) if mirrored else j)
        return carry

    lax.fori_loop(0, R, assemble, 0)
    if mirrored:
        def assemble_spare(n, carry):
            put(spare[n], 2 * n, 2 * n + 1)
            return carry

        lax.fori_loop(0, Z, assemble_spare, 0)
    my_rows = pl.ds(pl.multiple_of(row * height, height), height)
    my_cols = pl.ds(pl.multiple_of(col * width, width), width)
    statistic = 0.9 * stat_ref[...] + outer(my_rows, my_cols)
    stat_out[...] = statistic
    total = jnp.sum(jnp.sum(acc[...], axis=0, keepdims=True), axis=1, keepdims=True)
    scale = 0.5 / jnp.sqrt(total / side)

    for store, kept in ((l_hi, s_hi), (l_lo, s_lo)):
        store[:height, :] = kept[my_rows, :]
        store[height:, :] = kept[my_cols, :]

    left_rows = height + width
    line = lax.broadcasted_iota(jnp.int32, (left_rows, width), 0)
    line = jnp.where(line < height, row * height + line, col * width + line - height)
    across = lax.broadcasted_iota(jnp.int32, (left_rows, width), 1)

    def square(j, carry):
        there = pl.ds(pl.multiple_of(j * width, width), width)
        value = dot3((l_hi[...], l_lo[...]), (s_hi[:, there], s_lo[:, there]), ((1,), (0,)))
        panel = l_hi[:, there].astype(jnp.float32) + l_lo[:, there].astype(jnp.float32)
        ident = jnp.where(line == across + j * width, 0.84375, 0.0)
        quad = (0.25 * scale * scale) * value - (1.125 * scale) * panel + ident
        high, low = split(quad)
        q_hi[:, there] = high
        q_lo[:, there] = low
        return carry

    lax.fori_loop(0, C, square, 0)
    root = dot3(
        (q_hi[:height, :], q_lo[:height, :]), (q_hi[height:, :], q_lo[height:, :]), ((1,), (1,))
    )
    rows = row * height + lax.broadcasted_iota(jnp.int32, (height, width), 0)
    cols = col * width + lax.broadcasted_iota(jnp.int32, (height, width), 1)
    root_out[...] = (
        root - (0.5390625 * scale) * statistic + jnp.where(rows == cols, 1.5380859375, 0.0)
    )
    for copy, more, wanted in started:
        copy.wait_send()
        if mirrored:
            pl.when(wanted)(more.wait_send)


def local(R, C, gradient, stat_old):
    height, width = stat_old.shape
    mirrored = mirror(R, C, height, width)
    turned = gradient.T
    main = stat_old
    if mirrored:
        pick = chosen(lax.axis_index("gx"), lax.axis_index("gy"))
        main = jnp.where(pick == 0, stat_old[:, :height], stat_old[:, height:])
    pay = jnp.concatenate([main, turned], axis=0)
    payload = pay.shape[0]
    side, depth = R * height, C * gradient.shape[1]
    Z, X, Y = R // 2, 2, C // 2
    chips = Z * X * Y
    sends = 2 * (Z - 1) + 2 * Z + Z * (Y - 1) + (3 * Z) * (Y - 1) + 2 * chips
    half = jnp.bfloat16
    vmem = pl.BlockSpec(memory_space=pltpu.VMEM)
    return pl.pallas_call(
        functools.partial(kernel, R, C),
        out_shape=(jax.ShapeDtypeStruct(stat_old.shape, jnp.float32),) * 2,
        in_specs=[vmem] * 2,
        out_specs=(vmem,) * 2,
        scratch_shapes=[
            pltpu.VMEM((C, R, payload, height), jnp.float32),
            pltpu.VMEM((Z, height, height), jnp.float32),
            pltpu.VMEM((3 * depth, side), half),
            pltpu.VMEM((side, 3 * depth), half),
            pltpu.VMEM((side, side), half),
            pltpu.VMEM((side, side), half),
            pltpu.VMEM((height + width, side), half),
            pltpu.VMEM((height + width, side), half),
            pltpu.VMEM((height + width, side), half),
            pltpu.VMEM((height + width, side), half),
            pltpu.VMEM((height, height), jnp.float32),
            pltpu.SemaphoreType.DMA((sends,)),
            pltpu.SemaphoreType.DMA((2 * chips,)),
            pltpu.SemaphoreType.DMA((2 * chips,)),
            pltpu.SemaphoreType.DMA((2,)),
            pltpu.SemaphoreType.DMA((sends if mirrored else 1,)),
            pltpu.SemaphoreType.DMA((2 * Z,)),
            pltpu.SemaphoreType.DMA((2 * Z,)),
        ],
        compiler_params=pltpu.CompilerParams(collective_id=0, has_side_effects=True),
    )(pay, stat_old)


def solution(mesh):
    return jax.shard_map(
        functools.partial(local, mesh.shape["gx"], mesh.shape["gy"]),
        mesh=mesh,
        in_specs=(P("gx", "gy"), P("gx", "gy")),
        out_specs=(P("gx", "gy"), P("gx", "gy")),
        check_vma=False,
    )
```

```python
import functools

import jax
import jax.numpy as jnp
from jax import lax
from jax.experimental import pallas as pl
from jax.experimental.pallas import tpu as pltpu
from jax.sharding import PartitionSpec as P

MESH = pl.DeviceIdType.MESH
BOTH = 2


def split(value):
    high = value.astype(jnp.bfloat16)
    return high, (value - high.astype(jnp.float32)).astype(jnp.bfloat16)


def dot3(left, right, dims):
    def one(a, b):
        return lax.dot_general(a, b, (dims, ((), ())), preferred_element_type=jnp.float32)

    return one(left[0], right[0]) + (one(left[0], right[1]) + one(left[1], right[0]))


def mirror(R, C, height, width):
    return width == 2 * height and R == 2 * C


def chosen(i, j):
    odd = i % 2
    return jnp.where(i >= 2 * j, odd, 1 - odd)


def kernel(
    R, C, pay_ref, stat_ref, stat_out, root_out,
    buf, spare, gt, g, s_hi, s_lo, l_hi, l_lo, q_hi, q_lo, acc,
    send_sem, recv_sem, pair_sem, own_sem, spare_send, spare_recv, spare_pair,
):
    height, width = stat_ref.shape
    payload = pay_ref.shape[0]
    side = R * height
    mirrored = mirror(R, C, height, width)
    X, Z, Y = 2, R // 2, C // 2
    row, col = lax.axis_index("gx"), lax.axis_index("gy")
    z, x, y, core = row // X, row % X, col // 2, col % 2
    x_other = 1 - x
    z_at = [z] + [lax.rem(z + k, Z) for k in range(1, Z)]
    y_at = [y] + [lax.rem(y + k, Y) for k in range(1, Y)]
    z_order = [k for pair in zip(range(1, Z), range(Z - 1, 0, -1)) for k in pair]
    z_order = list(dict.fromkeys(z_order))

    barrier = pltpu.get_barrier_semaphore()
    peers = [(z_at[k] * X + x, col) for k in range(1, Z)]
    peers += [(z * X + x_other, col)]
    peers += [(row, y_at[k] * 2 + core) for k in range(1, Y)]
    peers += [(row, y * 2 + (1 - core))]
    for peer in peers:
        pl.semaphore_signal(barrier, inc=1, device_id=peer, device_id_type=MESH)
    pl.semaphore_wait(barrier, len(peers))

    started = []

    def lines(h, total):
        return pl.ds(0, total) if h == BOTH else pl.ds(h * (total // 2), total // 2)

    def place(zz, xx, yy, cc, h):
        return buf.at[yy * 2 + cc, zz * X + xx, lines(h, payload), :]

    def slot(zz, xx, yy, h):
        return (((h % BOTH) * Z + zz) * X + xx) * Y + yy

    def both(zz, xx, yy, cc):
        return jnp.logical_and(xx == 0, yy * 2 + cc == zz)

    def spare_place(zz, h):
        return spare.at[zz, lines(h, height), :]

    def send(src, zz, xx, yy, h, peer, pair=False):
        copy = pltpu.make_async_remote_copy(
            src_ref=src,
            dst_ref=place(zz, xx, yy, core, h),
            send_sem=send_sem.at[len(started)],
            recv_sem=(pair_sem if pair else recv_sem).at[slot(zz, xx, yy, h)],
            device_id=peer,
            device_id_type=MESH,
        )
        copy.start()
        more = None
        if mirrored:
            own = src_is_own[0]
            start = (
                stat_ref.at[lines(h, height), pl.ds(height, height)]
                if own
                else spare_place(zz, h)
            )
            more = pltpu.make_async_remote_copy(
                src_ref=start,
                dst_ref=spare_place(zz, h),
                send_sem=spare_send.at[len(started)],
                recv_sem=(spare_pair if pair else spare_recv).at[(h % BOTH) * Z + zz],
                device_id=peer,
                device_id_type=MESH,
            )
            pl.when(both(zz, xx, yy, core))(more.start)
        started.append((copy, more, both(zz, xx, yy, core)))

    src_is_own = [False]

    def source(zz, xx, yy, h, own):
        src_is_own[0] = own
        return pay_ref.at[lines(h, payload), :] if own else place(zz, xx, yy, core, h)

    def to_x(zz, yy, h, own=False):
        send(source(zz, x, yy, h, own), zz, x, yy, h, (z * X + x_other, col))

    def to_y(zz, xx, h, own=False):
        for k in range(1, Y):
            send(source(zz, xx, y, h, own), zz, xx, y, h, (row, y_at[k] * 2 + core))

    def to_pair(zz, xx, yy, h, own=False):
        send(source(zz, xx, yy, h, own), zz, xx, yy, h, (row, y * 2 + (1 - core)), True)

    def arrived(zz, xx, yy, cc, h, sem):
        here = place(zz, xx, yy, cc, h)
        pltpu.make_async_copy(here, here, sem.at[slot(zz, xx, yy, h)]).wait()
        if mirrored:
            there = spare_place(zz, h)
            sems = spare_pair if sem is pair_sem else spare_recv
            more = pltpu.make_async_copy(there, there, sems.at[(h % BOTH) * Z + zz])
            pl.when(both(zz, xx, yy, cc))(more.wait)

    own_copy = pltpu.make_async_copy(pay_ref, buf.at[col, row], own_sem.at[0])
    own_copy.start()
    if mirrored:
        own_more = pltpu.make_async_copy(
            stat_ref.at[:, pl.ds(height, height)], spare.at[z], own_sem.at[1]
        )
        pl.when(both(z, x, y, core))(own_more.start)
    to_x(z, y, BOTH, True)
    to_y(z, x, BOTH, True)
    for k in z_order:
        send(source(z, x, y, BOTH, True), z, x, y, BOTH, (z_at[k] * X + x, col))
    to_pair(z, x, y, BOTH, True)

    def second_leg(zz):
        arrived(zz, x_other, y, core, BOTH, recv_sem)
        to_y(zz, x_other, 0)
        for k in range(1, Y):
            arrived(zz, x, y_at[k], core, BOTH, recv_sem)
            to_x(zz, y_at[k], 1)
            to_pair(zz, x, y_at[k], BOTH)
        to_pair(zz, x_other, y, BOTH)

    second_leg(z)
    for k in z_order:
        zz = z_at[k]
        arrived(zz, x, y, core, BOTH, recv_sem)
        to_x(zz, y, BOTH)
        to_y(zz, x, BOTH)
        to_pair(zz, x, y, BOTH)
    for k in z_order:
        second_leg(z_at[k])
    for k in [0] + z_order:
        zz = z_at[k]
        for n in range(1, Y):
            for h in range(2):
                arrived(zz, x_other, y_at[n], core, h, recv_sem)
            to_pair(zz, x_other, y_at[n], BOTH)
    for k in [0] + z_order:
        for xx in range(X):
            for yy in range(Y):
                arrived(z_at[k], xx, yy, 1 - core, BOTH, pair_sem)
    own_copy.wait()
    if mirrored:
        pl.when(both(z, x, y, core))(own_more.wait)

    step = payload - height
    depth = C * step
    for i in range(R):
        for j in range(C):
            at = j * step
            here = slice(i * height, (i + 1) * height)
            high, low = split(buf[j, i, height:, :])
            gt[at:at + step, here] = high
            gt[depth + at:depth + at + step, here] = low
            gt[2 * depth + at:2 * depth + at + step, here] = high

    def turn(i, carry):
        here = pl.ds(pl.multiple_of(i * height, height), height)
        high = gt[:depth, here].T
        g[here, :depth] = high
        g[here, depth:2 * depth] = high
        g[here, 2 * depth:] = gt[depth:2 * depth, here].T
        return carry

    lax.fori_loop(0, R, turn, 0)

    def outer(here, there):
        return jnp.dot(g[here, :], gt[:, there], preferred_element_type=jnp.float32) * (1.0 / depth)

    acc[...] = jnp.zeros_like(acc)

    def put(value, a, b):
        here = pl.ds(pl.multiple_of(a * height, height), height)
        there = pl.ds(pl.multiple_of(b * height, height), height)
        value = 0.9 * value + outer(here, there)
        times = jnp.where(a == b, 1.0, 2.0) if mirrored else 1.0
        acc[...] += times * (value * value)
        high, low = split(value)
        s_hi[here, there] = high
        s_lo[here, there] = low
        if mirrored:
            s_hi[there, here] = high.T
            s_lo[there, here] = low.T

    def assemble(i, carry):
        for j in range(C):
            put(buf[j, i, :height, :], i, 2 * j + chosen(i, j) if mirrored else j)
        return carry

    lax.fori_loop(0, R, assemble, 0)
    if mirrored:
        def assemble_spare(n, carry):
            put(spare[n], 2 * n, 2 * n + 1)
            return carry

        lax.fori_loop(0, Z, assemble_spare, 0)
    my_rows = pl.ds(pl.multiple_of(row * height, height), height)
    my_cols = pl.ds(pl.multiple_of(col * width, width), width)
    statistic = 0.9 * stat_ref[...] + outer(my_rows, my_cols)
    stat_out[...] = statistic
    total = jnp.sum(jnp.sum(acc[...], axis=0, keepdims=True), axis=1, keepdims=True)
    scale = 0.5 / jnp.sqrt(total / side)

    for store, kept in ((l_hi, s_hi), (l_lo, s_lo)):
        store[:height, :] = kept[my_rows, :]
        store[height:, :] = kept[my_cols, :]

    left_rows = height + width
    line = lax.broadcasted_iota(jnp.int32, (left_rows, width), 0)
    line = jnp.where(line < height, row * height + line, col * width + line - height)
    across = lax.broadcasted_iota(jnp.int32, (left_rows, width), 1)

    def square(j, carry):
        there = pl.ds(pl.multiple_of(j * width, width), width)
        rounded = s_hi[:, there]
        value = jnp.dot(l_hi[...], rounded, preferred_element_type=jnp.float32)
        value += jnp.dot(l_lo[...], rounded, preferred_element_type=jnp.float32)
        panel = l_hi[:, there].astype(jnp.float32) + l_lo[:, there].astype(jnp.float32)
        ident = jnp.where(line == across + j * width, 0.84375, 0.0)
        quad = (0.25 * scale * scale) * value - (1.125 * scale) * panel + ident
        high, low = split(quad)
        q_hi[:, there] = high
        q_lo[:, there] = low
        return carry

    lax.fori_loop(0, C, square, 0)
    root = dot3(
        (q_hi[:height, :], q_lo[:height, :]), (q_hi[height:, :], q_lo[height:, :]), ((1,), (1,))
    )
    rows = row * height + lax.broadcasted_iota(jnp.int32, (height, width), 0)
    cols = col * width + lax.broadcasted_iota(jnp.int32, (height, width), 1)
    root_out[...] = (
        root - (0.5390625 * scale) * statistic + jnp.where(rows == cols, 1.5380859375, 0.0)
    )
    for copy, more, wanted in started:
        copy.wait_send()
        if mirrored:
            pl.when(wanted)(more.wait_send)


def local(R, C, gradient, stat_old):
    height, width = stat_old.shape
    mirrored = mirror(R, C, height, width)
    turned = gradient.T
    main = stat_old
    if mirrored:
        pick = chosen(lax.axis_index("gx"), lax.axis_index("gy"))
        main = jnp.where(pick == 0, stat_old[:, :height], stat_old[:, height:])
    pay = jnp.concatenate([main, turned], axis=0)
    payload = pay.shape[0]
    side, depth = R * height, C * gradient.shape[1]
    Z, X, Y = R // 2, 2, C // 2
    chips = Z * X * Y
    sends = (Z - 1) + Z + 3 * Z * (Y - 1) + chips
    half = jnp.bfloat16
    vmem = pl.BlockSpec(memory_space=pltpu.VMEM)
    return pl.pallas_call(
        functools.partial(kernel, R, C),
        out_shape=(jax.ShapeDtypeStruct(stat_old.shape, jnp.float32),) * 2,
        in_specs=[vmem] * 2,
        out_specs=(vmem,) * 2,
        scratch_shapes=[
            pltpu.VMEM((C, R, payload, height), jnp.float32),
            pltpu.VMEM((Z, height, height), jnp.float32),
            pltpu.VMEM((3 * depth, side), half),
            pltpu.VMEM((side, 3 * depth), half),
            pltpu.VMEM((side, side), half),
            pltpu.VMEM((side, side), half),
            pltpu.VMEM((height + width, side), half),
            pltpu.VMEM((height + width, side), half),
            pltpu.VMEM((height + width, side), half),
            pltpu.VMEM((height + width, side), half),
            pltpu.VMEM((height, height), jnp.float32),
            pltpu.SemaphoreType.DMA((sends,)),
            pltpu.SemaphoreType.DMA((2 * chips,)),
            pltpu.SemaphoreType.DMA((2 * chips,)),
            pltpu.SemaphoreType.DMA((2,)),
            pltpu.SemaphoreType.DMA((sends if mirrored else 1,)),
            pltpu.SemaphoreType.DMA((2 * Z,)),
            pltpu.SemaphoreType.DMA((2 * Z,)),
        ],
        compiler_params=pltpu.CompilerParams(collective_id=0, has_side_effects=True),
    )(pay, stat_old)


def solution(mesh):
    return jax.shard_map(
        functools.partial(local, mesh.shape["gx"], mesh.shape["gy"]),
        mesh=mesh,
        in_specs=(P("gx", "gy"), P("gx", "gy")),
        out_specs=(P("gx", "gy"), P("gx", "gy")),
        check_vma=False,
    )
```
